32 devices in a mesh: ep: 4 (over y, core), fsdp: 8 (over z, x).
Axes of the slice: x: 2, y: 2, z: 4, core: 2. Of those that a mesh axis runs over, the one named last changes fastest.
Arguments:
- w_down: float32 [16, 6400, 4096], P('ep', None, 'fsdp'), may hold values from -0.109375 to 0.109375
- router_weight: float32 [4096, 16], P('fsdp', 'ep'), may hold values from -0.09375 to 0.09375
- router_gain: float32 [4096], P('fsdp'), may hold values from 0.25 to 1.75
Outputs:
- serve_down: bfloat16 [16, 6400, 4096], P('ep', 'fsdp')
- scale_down: float32 [16, 6400], P('ep', 'fsdp')
- serve_router: bfloat16 [4096, 16], replicated
The draws below stay inside these ranges and needn't reach their ends.
All inputs are finite; a program needn't handle non-finite values.
Results may differ from the reference program's by a relative error of at most 0.001.
Values may be sent and summed in bfloat16 or wider, within the bound.
No kernel may reach another device: no remote copies, remote signals or barrier semaphores. Data moves between devices by JAX's collectives and lax.ppermute only.
A program may use at most 192 MiB of HBM per device.

```python
import jax
import jax.numpy as jnp
from jax import lax

EXPERTS = 16
D_MODEL = 4096
D_EXPERT = 6400


def strengthened(entries, key, source, target, parts, factor):
    def block_of(axis_at):
        return (jnp.arange(entries.shape[axis_at]) // (entries.shape[axis_at] // parts)).reshape((-1,) + (1,) * (entries.ndim - 1 - axis_at))

    near = jax.random.permutation(key, parts)[block_of(target)]
    second = (block_of(target) + parts // 2) % parts
    return jnp.where((block_of(source) == near) | (block_of(source) == second), factor * entries, entries)


def shard_levels(stream_key, extent, cuts, low, high):
    gain = 1.0
    for position, parts in cuts:
        heights = jax.random.uniform(jax.random.fold_in(jax.random.fold_in(stream_key, 6), position), (parts,), jnp.float32, low / len(cuts), high / len(cuts))
        gain = gain * jnp.repeat(jnp.exp(heights), extent[position] // parts).reshape((-1,) + (1,) * (len(extent) - 1 - position))
    return gain


def scatter_about(rng, extent, width, limit, pieces=(), held_as=jnp.bfloat16):
    entries = width * jax.random.normal(rng, extent, jnp.float32)
    if pieces:
        entries = entries * shard_levels(rng, extent, pieces, -0.22, 0.18)
    return jnp.clip(entries, -limit, limit).astype(held_as)


def heavy_noise(own_key, dims, deviation, limit, shards, heavy, held_as=jnp.bfloat16):
    array = deviation * jax.random.normal(own_key, dims, jnp.float32)
    if shards:
        array = array * shard_levels(own_key, dims, shards, -0.22, 0.18)
    return jnp.clip(strengthened(array, jax.random.fold_in(own_key, 3), *heavy), -limit, limit).astype(held_as)


def setup_inputs(seed: int = 0) -> dict:
    arg_keys = jax.random.split(jax.random.key(seed), 4)
    return {
        "w_down": heavy_noise(arg_keys[0], (EXPERTS, D_EXPERT, D_MODEL), D_EXPERT ** -0.5, 0.109375, ((0, 4), (2, 8)), (2, 1, 8, 2.0), jnp.float32),
        "router_weight": scatter_about(arg_keys[1], (D_MODEL, EXPERTS), D_MODEL ** -0.5, 0.09375, ((0, 8), (1, 4)), jnp.float32),
        "router_gain": jnp.clip(1.0 + 0.15 * jax.random.normal(arg_keys[2], (D_MODEL,), jnp.float32), 0.25, 1.75),
    }


def reference(w_down, router_weight, router_gain):
    scale_down = jnp.sqrt(lax.optimization_barrier(jnp.sum(w_down * w_down, axis=2)))
    serve_down = (w_down / jnp.expand_dims(scale_down, 2)).astype(jnp.bfloat16)
    serve_router = (router_weight * router_gain[:, None]).astype(jnp.bfloat16)
    return (serve_down, scale_down, serve_router)
```

```python
import functools

import jax
import jax.numpy as jnp
from jax import lax
from jax.experimental import pallas as pl
from jax.experimental.pallas import tpu as pltpu
from jax.sharding import PartitionSpec as P

LANES = 128


def tile_of(size, most):
    for rows in range(min(size, most), 15, -1):
        if size % rows == 0 and rows % 16 == 0:
            return rows
    return size


def narrow_kernel(count, me_ref, *refs):
    ws, invs, outs = refs[:count], refs[count : 2 * count], refs[2 * count :]
    for w, inv, out in zip(ws, invs, outs):
        factor = inv[0]
        for lane in range(0, out.shape[1], LANES):
            at = pl.ds(lane, LANES)
            out[:, at] = (w[0, 0, :, at] * factor).astype(out.dtype)


def narrow(w, inv, me, expert, start, size, hops, most=160):
    width = w.shape[3]
    rows = tile_of(size, most)
    first = start // rows
    in_specs = [
        pl.BlockSpec((1, 1, rows, width), lambda r, me, hop=hop: (expert, me[0] ^ hop, first + r, 0))
        for hop in hops
    ] + [
        pl.BlockSpec((1, rows, LANES), lambda r, me, hop=hop: (me[0] ^ hop, first + r, 0))
        for hop in hops
    ]
    out_specs = [pl.BlockSpec((rows, width), lambda r, me: (r, 0)) for _ in hops]
    elements = len(hops) * size * width
    return pl.pallas_call(
        functools.partial(narrow_kernel, len(hops)),
        grid_spec=pltpu.PrefetchScalarGridSpec(
            num_scalar_prefetch=1, grid=(size // rows,), in_specs=in_specs, out_specs=out_specs
        ),
        out_shape=[jax.ShapeDtypeStruct((size, width), jnp.bfloat16) for _ in hops],
        cost_estimate=pl.CostEstimate(flops=elements, bytes_accessed=6 * elements, transcendentals=0),
        name="narrow",
    )(me, *([w] * len(hops)), *([inv] * len(hops)))


def place_kernel(count, width, hops, me_ref, *refs):
    pieces, out = refs[:count], refs[-1]
    for hop, piece in zip(hops, pieces):
        source = me_ref[0] ^ hop
        out[0, :, pl.ds(pl.multiple_of(source * width, LANES), width)] = piece[...]


def place(pieces, held, me, shape, expert, start, size, hops, most=80):
    width = pieces[0].shape[1]
    rows = tile_of(size, most)
    first = start // rows
    in_specs = [pl.BlockSpec((rows, width), lambda r, me: (r, 0)) for _ in hops]
    operands = [me, *pieces]
    aliases = {}
    if held is not None:
        in_specs.append(pl.BlockSpec(memory_space=pl.ANY))
        aliases = {len(operands): 0}
        operands.append(held)
    elements = len(hops) * size * width
    return pl.pallas_call(
        functools.partial(place_kernel, len(hops), width, hops),
        grid_spec=pltpu.PrefetchScalarGridSpec(
            num_scalar_prefetch=1,
            grid=(size // rows,),
            in_specs=in_specs,
            out_specs=pl.BlockSpec((1, rows, shape[2]), lambda r, me: (expert, first + r, 0)),
        ),
        out_shape=jax.ShapeDtypeStruct(shape, jnp.bfloat16),
        input_output_aliases=aliases,
        cost_estimate=pl.CostEstimate(flops=elements, bytes_accessed=4 * elements, transcendentals=0),
        name="place",
    )(*operands)


def body(group, w_down, router_weight, router_gain):
    experts, inner, width = w_down.shape
    n = inner // group
    index = lax.axis_index("fsdp")
    me = jnp.full((1,), index, jnp.int32)

    router = (router_weight * router_gain[:, None]).astype(jnp.bfloat16)
    partial = jnp.sum(w_down * w_down, axis=2)
    packed = jnp.concatenate([partial.reshape(-1), router.T.astype(jnp.float32).reshape(-1)])
    gathered = lax.all_gather(packed, "fsdp")
    scale = jnp.sqrt(jnp.sum(gathered[:, : experts * inner], axis=0)).reshape(experts, inner)
    rows_router = gathered[:, experts * inner :].astype(jnp.bfloat16)
    rows_router = rows_router.reshape(group, router.shape[1], router.shape[0])
    rows_router = rows_router.transpose(1, 0, 2).reshape(router.shape[1], -1)
    serve_router = lax.all_gather(rows_router, "ep", axis=0, tiled=True).T

    scale_down = lax.dynamic_slice_in_dim(scale, index * n, n, axis=1)
    inverse = 1.0 / scale
    w = w_down.reshape(experts, group, n, width)

    hops = list(range(group - 1, -1, -1))
    shape = (experts, n, group * width)
    chunks = [(expert, 0, n) for expert in range(experts)]
    held = None
    landed = []
    for at, (expert, start, size) in enumerate(chunks):
        inv = jnp.broadcast_to(inverse[expert].reshape(group, n, 1), (group, n, LANES))
        pieces = narrow(w, inv, me, expert, start, size, hops)
        if at >= 2:
            pieces, landed[at - 2] = lax.optimization_barrier((pieces, landed[at - 2]))
        got = [
            lax.ppermute(piece, "fsdp", [(j, j ^ hop) for j in range(group)]) if hop else piece
            for hop, piece in zip(hops, pieces)
        ]
        landed.append(got)
    for (expert, start, size), got in zip(chunks, landed):
        held = place(got, held, me, shape, expert, start, size, hops)
    return (held, scale_down, serve_router)


def solution(mesh):
    in_specs = (P("ep", None, "fsdp"), P("fsdp", "ep"), P("fsdp"))
    out_specs = (P("ep", "fsdp", None), P("ep", "fsdp"), P())
    return jax.shard_map(
        functools.partial(body, mesh.shape["fsdp"]),
        mesh=mesh,
        in_specs=in_specs,
        out_specs=out_specs,
        check_vma=False,
    )
```
